8 devices in a mesh: data: 1 (over z), outer: 2 (over y), expert: 4 (over x, core).
Axes of the slice: x: 2, y: 2, z: 1, core: 2. Of those that a mesh axis runs over, the one named last changes fastest.
Arguments:
- x_disp: bfloat16 [8, 40, 32, 1536], P('data', ('outer', 'expert'))
- w_gate: bfloat16 [40, 1536, 512], P(('outer', 'expert'))
- w_up: bfloat16 [40, 1536, 512], P(('outer', 'expert'))
- w_down: bfloat16 [40, 512, 1536], P(('outer', 'expert'))
- slot_idx: int32 [1280, 8], P(('data', 'outer', 'expert'))
- expert_ids: int32 [1280, 8], P(('data', 'outer', 'expert'))
- gate_wts: float32 [1280, 8], P(('data', 'outer', 'expert'))
Outputs:
- output: bfloat16 [1280, 1536], P(('data', 'outer', 'expert'))
All inputs are finite; a program needn't handle non-finite values.
Results may differ from the reference program's by a relative error of at most 0.00823053.
Values are sent between devices in bfloat16 or wider.
A program may use at most 1 GiB of HBM per device.

```python
import jax
import jax.numpy as jnp
from jax import lax

D = 1536
FF = 512
EXPERTS = 40
TOP = 8
CAP = 32
OUTER = 2
INNER = 4
NODE_MAX = 1
TOK = 160

GROUP_DEVS = OUTER * INNER
TOKENS = GROUP_DEVS * TOK
BLOCK_EXPERTS = EXPERTS // OUTER
BONUS = 2 ** 20


def draw_routing(key):
    key_hot, key_block, key_noise, key_bias = jax.random.split(key, 4)
    hot_expert = jax.random.randint(key_hot, (), 0, EXPERTS)
    forced = (jnp.arange(TOKENS) % TOK < CAP)[:, None]
    blocks = jnp.arange(OUTER)
    block_score = jax.random.randint(key_block, (TOKENS, OUTER), 0, 1024) * OUTER + blocks
    block_score = block_score + jnp.where(forced & (blocks == hot_expert // BLOCK_EXPERTS), BONUS, 0)
    best_blocks = jnp.argsort(-block_score, axis=1)[:, :NODE_MAX]
    chosen = jnp.any(best_blocks[:, :, None] == blocks[None, None, :], axis=1)
    experts = jnp.arange(EXPERTS)
    expert_bias = jax.random.randint(key_bias, (EXPERTS,), 0, 1024)
    rand_noise = jax.random.randint(key_noise, (TOKENS, EXPERTS), 0, 1024)
    expert_score = ((rand_noise + expert_bias) * EXPERTS + experts).reshape(TOKENS, OUTER, BLOCK_EXPERTS)
    block_best = expert_score == jnp.max(expert_score, axis=2, keepdims=True)
    expert_score = jnp.where(chosen[:, :, None], expert_score + jnp.where(block_best, BONUS, 0), -1)
    expert_score = expert_score.reshape(TOKENS, EXPERTS) + jnp.where(forced & (experts == hot_expert), 2 * BONUS, 0)
    expert_ids = jnp.sort(jnp.argsort(-expert_score, axis=1)[:, :TOP], axis=1)
    source = jnp.arange(TOKENS) // TOK
    group_id = (source[:, None] * EXPERTS + expert_ids).reshape(-1)
    sort_order = jnp.argsort(group_id, stable=True)
    counts = jnp.zeros(GROUP_DEVS * EXPERTS, jnp.int32).at[group_id].add(1)
    starts = jnp.cumsum(counts) - counts
    sorted_rank = jnp.arange(TOKENS * TOP) - starts[group_id[sort_order]]
    slot_rank = jnp.zeros(TOKENS * TOP, jnp.int32).at[sort_order].set(sorted_rank.astype(jnp.int32))
    slot_idx = jnp.where(slot_rank < CAP, slot_rank, -1).reshape(TOKENS, TOP)
    return slot_idx.astype(jnp.int32), expert_ids.astype(jnp.int32)


def setup_inputs(seed: int = 0, part: int = 0) -> dict:
    base_key = jax.random.key(seed)
    key_wg, key_wu, key_wd = jax.random.split(base_key, 3)
    part_key = jax.random.fold_in(base_key, part)
    key_x, key_route, key_gate = jax.random.split(part_key, 3)
    x_disp = jax.random.normal(key_x, (GROUP_DEVS, EXPERTS, CAP, D), jnp.float32).astype(jnp.bfloat16)
    w_gate = (jax.random.normal(key_wg, (EXPERTS, D, FF), jnp.float32) * D ** -0.5).astype(jnp.bfloat16)
    w_up = (jax.random.normal(key_wu, (EXPERTS, D, FF), jnp.float32) * D ** -0.5).astype(jnp.bfloat16)
    w_down = (jax.random.normal(key_wd, (EXPERTS, FF, D), jnp.float32) * FF ** -0.5).astype(jnp.bfloat16)
    slot_idx, expert_ids = draw_routing(key_route)
    gate_wts = jax.nn.softmax(1.5 * jax.random.normal(key_gate, (TOKENS, TOP), jnp.float32), axis=1)
    return {"x_disp": x_disp, "w_gate": w_gate, "w_up": w_up, "w_down": w_down, "slot_idx": slot_idx, "expert_ids": expert_ids, "gate_wts": gate_wts}


def expert_ffn(expert_args):
    rows_e, gate_e, up_e, down_e = expert_args
    gate_proj = jnp.dot(rows_e, gate_e, preferred_element_type=jnp.float32)
    up_proj = jnp.dot(rows_e, up_e, preferred_element_type=jnp.float32)
    hidden = (jax.nn.silu(gate_proj) * up_proj).astype(jnp.bfloat16)
    return jnp.dot(hidden, down_e, preferred_element_type=jnp.float32).astype(jnp.bfloat16)


def reference(x_disp, w_gate, w_up, w_down, slot_idx, expert_ids, gate_wts):
    x_rows = jnp.transpose(x_disp, (1, 0, 2, 3)).reshape(EXPERTS, GROUP_DEVS * CAP, D)
    y_out = lax.map(expert_ffn, (x_rows, w_gate, w_up, w_down))
    y_flat = y_out.reshape(EXPERTS * GROUP_DEVS * CAP, D)
    source = jnp.arange(TOKENS) // TOK
    kept_mask = slot_idx >= 0
    flat_idx = jnp.where(kept_mask, (expert_ids * GROUP_DEVS + source[:, None]) * CAP + slot_idx, 0)
    weight = jnp.where(kept_mask, gate_wts, 0.0)

    def combine(source_args):
        pick_idx, pick_wts = source_args
        picked = jnp.take(y_flat, pick_idx, axis=0).astype(jnp.float32)
        return jnp.sum(picked * pick_wts[:, :, None], axis=1).astype(jnp.bfloat16)

    combined = lax.map(combine, (flat_idx.reshape(GROUP_DEVS, TOK, TOP), weight.reshape(GROUP_DEVS, TOK, TOP)))
    return combined.reshape(TOKENS, D)
```

```python
import functools

import jax
import jax.numpy as jnp
from jax import lax
from jax.experimental import pallas as pl
from jax.experimental.pallas import tpu as pltpu
from jax.sharding import PartitionSpec as P

XW = 640
GROUPS = ((640, 384), (1024, 256), (1280, 256))
BF16_MAX = 3.3895313892515355e38


def kernel(x_hbm, wg_hbm, wu_hbm, wd_hbm, slot_ref, ids_ref, gate_ref, out_ref,
           x_v, wg_v, wu_v, wd_v, h_v, y_send, r_x, r_y, tok, tok_r, st_f32,
           s_mat, used, z_send, z_recv, w_send, w_recv, acc,
           in_sems, tok_ssem, tok_rsem, x_ssem, x_rsem, y_ssem, y_rsem,
           z_ssem, z_rsem, w_ssem, w_rsem):
    b = lax.axis_index("outer")
    q = lax.axis_index("expert")
    x = q // 2
    c = q % 2
    experts = x_v.shape[0]
    cap = x_v.shape[2]
    blk = experts * cap
    toks = out_ref.shape[0]

    def dev(bb, xx, cc):
        return {"outer": bb, "expert": 2 * xx + cc}

    row = [(b, x, c), (b, x, 1 - c), (b, 1 - x, c), (b, 1 - x, 1 - c)]
    col = [(b, x, c), (b, x, 1 - c), (1 - b, x, c), (1 - b, x, 1 - c)]
    x_partner = dev(b, 1 - x, c)
    y_partner = dev(1 - b, x, c)

    def in_copies(e):
        return (pltpu.make_async_copy(x_hbm.at[:, e], x_v.at[e], in_sems.at[0, e]),
                pltpu.make_async_copy(wg_hbm.at[e], wg_v.at[e], in_sems.at[1, e]),
                pltpu.make_async_copy(wu_hbm.at[e], wu_v.at[e], in_sems.at[2, e]),
                pltpu.make_async_copy(wd_hbm.at[e], wd_v.at[e], in_sems.at[3, e]))

    def remote(src, dst, ssem, rsem, device):
        return pltpu.make_async_remote_copy(
            src_ref=src, dst_ref=dst, send_sem=ssem, recv_sem=rsem,
            device_id=device, device_id_type=pl.DeviceIdType.MESH)

    def x_copy(k, e):
        _, xx, cc = row[k]
        return remote(y_send.at[e, :, xx, cc, :, pl.ds(0, XW)], r_x.at[:, k, e],
                      x_ssem.at[k, e], x_rsem.at[k, e], dev(*row[k]))

    def y_copy(g, k, e):
        bb, _, cc = col[k]
        start, width = GROUPS[g]
        return remote(y_send.at[e, bb, :, cc, :, pl.ds(start, width)],
                      r_y.at[:, k, e, :, pl.ds(start - XW, width)],
                      y_ssem.at[g, k, e], y_rsem.at[g, k, e], dev(*col[k]))

    def z_copy(g):
        start, width = GROUPS[g]
        cols = pl.ds(start - XW, width)
        return remote(z_send.at[:, cols], z_recv.at[:, cols], z_ssem.at[g], z_rsem.at[g], x_partner)

    w_copy = remote(w_send, w_recv, w_ssem, w_rsem, y_partner)
    tok_copies = [remote(tok, tok_r.at[0], tok_ssem.at[0], tok_rsem.at[0], x_partner),
                  remote(tok, tok_r.at[1], tok_ssem.at[1], tok_rsem.at[1], y_partner)]

    for e in range(2):
        for cp in in_copies(e):
            cp.start()

    barrier = pltpu.get_barrier_semaphore()
    for peer in (row[1], row[2], row[3], col[2], col[3]):
        pl.semaphore_signal(barrier, inc=1, device_id=dev(*peer), device_id_type=pl.DeviceIdType.MESH)

    slot = slot_ref[...]
    flat = jnp.where(slot >= 0, ids_ref[...] * cap + slot, -1).astype(jnp.float32)
    tok[...] = jnp.full(tok.shape, -1.0, jnp.float32)
    tok[0:8, 0:toks] = flat
    tok[8:16, 0:toks] = gate_ref[...]

    pl.semaphore_wait(barrier, 5)
    for cp in tok_copies:
        cp.start()

    def ffn(e, carry):
        for cp in in_copies(e):
            cp.wait()

        @pl.when(e + 2 < experts)
        def _():
            for cp in in_copies(e + 2):
                cp.start()

        xs = x_v[e].reshape(8 * cap, x_v.shape[3])
        ff = h_v.shape[1]
        for n in range(0, ff, 256):
            g = jnp.dot(xs, wg_v[e, :, n:n + 256], preferred_element_type=jnp.float32)
            u = jnp.dot(xs, wu_v[e, :, n:n + 256], preferred_element_type=jnp.float32)
            h_v[:, n:n + 256] = (jax.nn.silu(g) * u).astype(jnp.bfloat16)
        h = h_v[...]
        for n in range(0, y_send.shape[5], 256):
            y = jnp.dot(h, wd_v[e, :, n:n + 256], preferred_element_type=jnp.float32)
            y_send[e, :, :, :, :, n:n + 256] = y.astype(jnp.bfloat16).reshape(2, 2, 2, cap, 256)
        r_x[:, 0, e] = y_send[e, :, x, c, :, 0:XW]
        r_y[:, 0, e] = y_send[e, b, :, c, :, XW:]
        for k in (2, 3, 1):
            x_copy(k, e).start()
            y_copy(0, k, e).start()
        return carry

    lax.fori_loop(0, experts, ffn, 0)

    for g in range(1, len(GROUPS)):
        for e in range(experts):
            for k in (2, 3, 1):
                y_copy(g, k, e).start()

    def build(i, tok_val, devices):
        rows = lax.broadcasted_iota(jnp.int32, (blk, tok_val.shape[1]), 0)
        for k in range(4):
            bb, xx, cc = devices[k]
            want = (rows + blk * (4 * bb + 2 * xx + cc)).astype(jnp.float32)
            s = jnp.zeros(want.shape, jnp.float32)
            for j in range(8):
                s = s + jnp.where(tok_val[j:j + 1, :] == want, tok_val[8 + j:9 + j, :], 0.0)
            st_f32[k * blk:(k + 1) * blk, :] = s
            hit = jnp.max(s, axis=1, keepdims=True)
            used[i, k * blk:(k + 1) * blk, :] = jnp.broadcast_to(
                jnp.where(hit > 0.0, 1.0, 0.0), (blk, 128)).astype(jnp.bfloat16)
        for m in range(0, 4 * blk, 128):
            t = jnp.transpose(st_f32[m:m + 128, :])[0:toks, :]
            s1 = jnp.minimum(t, BF16_MAX).astype(jnp.bfloat16)
            t = t - s1.astype(jnp.float32)
            s2 = t.astype(jnp.bfloat16)
            s3 = (t - s2.astype(jnp.float32)).astype(jnp.bfloat16)
            s_mat[i, 0:toks, m:m + 128] = s1
            s_mat[i, toks:2 * toks, m:m + 128] = s2
            s_mat[i, 2 * toks:3 * toks, m:m + 128] = s3

    def combine(i, rows, start, write):
        width = rows.shape[4]
        for n in range(0, width, 128):
            r = rows[:, :, :, :, n:n + 128].reshape(4 * blk, 128)
            r = jnp.where(used[i] > 0, r, jnp.zeros_like(r))
            o = jnp.dot(s_mat[i], r, preferred_element_type=jnp.float32)
            write(start + n, o[0:toks] + o[toks:2 * toks] + o[2 * toks:3 * toks])

    for cp in tok_copies:
        cp.wait_recv()
    build(0, tok_r[0], col)
    build(1, tok[...], col)
    build(2, tok_r[1], row)
    build(3, tok[...], row)

    def put_z(n, v):
        z_send[:, n:n + 128] = v

    def put_w(n, v):
        w_send[:, n:n + 128] = v.astype(jnp.bfloat16)

    def put_acc(n, v):
        acc[:, n:n + 128] = v

    def y_group(g):
        start, width = GROUPS[g]
        cols = pl.ds(start - XW, width)
        for e in range(experts):
            for k in (1, 2, 3):
                y_copy(g, k, e).wait_recv()
        combine(0, r_y.at[pl.ds(1 - x, 1), :, :, :, cols], start - XW, put_z)
        z_copy(g).start()
        combine(1, r_y.at[pl.ds(x, 1), :, :, :, cols], start, put_acc)

    y_group(0)
    y_group(1)
    for e in range(experts):
        for k in (1, 2, 3):
            x_copy(k, e).wait_recv()
    combine(2, r_x.at[pl.ds(1 - b, 1)], 0, put_w)
    w_copy.start()
    combine(3, r_x.at[pl.ds(b, 1)], 0, put_acc)
    y_group(2)

    for g, (start, width) in enumerate(GROUPS):
        z_copy(g).wait_recv()
        out_ref[:, start:start + width] = (
            acc[:, start:start + width] + z_recv[:, start - XW:start - XW + width]).astype(jnp.bfloat16)
    w_copy.wait_recv()
    out_ref[:, 0:XW] = (acc[:, 0:XW] + w_recv[...].astype(jnp.float32)).astype(jnp.bfloat16)

    for cp in tok_copies:
        cp.wait_send()
    for e in range(experts):
        for k in (1, 2, 3):
            x_copy(k, e).wait_send()
            for g in range(len(GROUPS)):
                y_copy(g, k, e).wait_send()
    for g in range(len(GROUPS)):
        z_copy(g).wait_send()
    w_copy.wait_send()


def solution(mesh):
    def local_step(x_disp, w_gate, w_up, w_down, slot_idx, expert_ids, gate_wts):
        sources, experts, cap, width = x_disp.shape
        ff = w_gate.shape[2]
        toks = slot_idx.shape[0]
        yw = width - XW
        ng = len(GROUPS)
        dma = pltpu.SemaphoreType.DMA
        bf16, f32 = jnp.bfloat16, jnp.float32
        vmem = pl.BlockSpec(memory_space=pltpu.VMEM)
        hbm = pl.BlockSpec(memory_space=pl.ANY)
        rows = 4 * experts * cap
        return pl.pallas_call(
            kernel,
            out_shape=jax.ShapeDtypeStruct((toks, width), bf16),
            in_specs=[hbm] * 4 + [vmem] * 3,
            out_specs=vmem,
            scratch_shapes=[
                pltpu.VMEM((experts, sources, cap, width), bf16),
                pltpu.VMEM((experts, width, ff), bf16),
                pltpu.VMEM((experts, width, ff), bf16),
                pltpu.VMEM((experts, ff, width), bf16),
                pltpu.VMEM((sources * cap, ff), bf16),
                pltpu.VMEM((experts, 2, 2, 2, cap, width), bf16),
                pltpu.VMEM((2, 4, experts, cap, XW), bf16),
                pltpu.VMEM((2, 4, experts, cap, yw), bf16),
                pltpu.VMEM((16, 256), f32),
                pltpu.VMEM((2, 16, 256), f32),
                pltpu.VMEM((rows, 256), f32),
                pltpu.VMEM((4, 3 * toks, rows), bf16),
                pltpu.VMEM((4, rows, 128), bf16),
                pltpu.VMEM((toks, yw), f32),
                pltpu.VMEM((toks, yw), f32),
                pltpu.VMEM((toks, XW), bf16),
                pltpu.VMEM((toks, XW), bf16),
                pltpu.VMEM((toks, width), f32),
                dma((4, experts)), dma((2,)), dma((2,)),
                dma((4, experts)), dma((4, experts)),
                dma((ng, 4, experts)), dma((ng, 4, experts)),
                dma((ng,)), dma((ng,)), dma, dma,
            ],
            compiler_params=pltpu.CompilerParams(
                collective_id=0, has_side_effects=True, vmem_limit_bytes=60 * 2**20),
            name="moe",
        )(x_disp, w_gate, w_up, w_down, slot_idx.T, expert_ids.T, gate_wts.T)

    expert_spec = P(("outer", "expert"))
    token_spec = P(("data", "outer", "expert"))
    return jax.shard_map(local_step, mesh=mesh, in_specs=(P("data", ("outer", "expert")), expert_spec, expert_spec, expert_spec, token_spec, token_spec, token_spec), out_specs=token_spec, check_vma=False)
```

```python
import functools

import jax
import jax.numpy as jnp
from jax import lax
from jax.experimental import pallas as pl
from jax.experimental.pallas import tpu as pltpu
from jax.sharding import PartitionSpec as P

XW = 640
GROUPS = ((640, 384), (1024, 256), (1280, 128), (1408, 128))
TILE = 256
BF16_MAX = 3.3895313892515355e38


def kernel(x_hbm, wg_hbm, wu_hbm, wd_hbm, slot_hbm, ids_hbm, gate_hbm, out_ref,
           slot_ref, ids_ref, gate_ref, x_v, wg_v, wu_v, wd_v, h_v, y_send, r_x, r_y, tok, tok_r, st_f32,
           s_mat, used, z_send, z_recv, w_send, w_recv, acc,
           in_sems, half_sems, map_sems, tok_ssem, tok_rsem, x_ssem, x_rsem, y_ssem, y_rsem,
           z_ssem, z_rsem, w_ssem, w_rsem):
    b = lax.axis_index("outer")
    q = lax.axis_index("expert")
    x = q // 2
    c = q % 2
    experts = x_v.shape[0]
    cap = x_v.shape[2]
    blk = experts * cap
    toks = out_ref.shape[0]

    def dev(bb, xx, cc):
        return {"outer": bb, "expert": 2 * xx + cc}

    row = [(b, x, c), (b, x, 1 - c), (b, 1 - x, c), (b, 1 - x, 1 - c)]
    col = [(b, x, c), (b, x, 1 - c), (1 - b, x, c), (1 - b, x, 1 - c)]
    x_partner = dev(b, 1 - x, c)
    y_partner = dev(1 - b, x, c)

    def rows_in(e):
        return pltpu.make_async_copy(x_hbm.at[:, e], x_v.at[e], in_sems.at[0, e % 2])

    def down_in(e):
        return pltpu.make_async_copy(wd_hbm.at[e], wd_v.at[e], in_sems.at[3, e % 2])

    def in_copies(e):
        return (rows_in(e),
                pltpu.make_async_copy(wg_hbm.at[e], wg_v.at[e], in_sems.at[1, e % 2]),
                pltpu.make_async_copy(wu_hbm.at[e], wu_v.at[e], in_sems.at[2, e % 2]),
                down_in(e))

    def remote(src, dst, ssem, rsem, device):
        return pltpu.make_async_remote_copy(
            src_ref=src, dst_ref=dst, send_sem=ssem, recv_sem=rsem,
            device_id=device, device_id_type=pl.DeviceIdType.MESH)

    def drain(ref, sem):
        pltpu.make_async_copy(ref, ref, sem).wait()

    others = pl.ds(1, 3)

    def x_copy(k, e):
        _, xx, cc = row[k]
        return remote(y_send.at[e, :, xx, cc, :, pl.ds(0, XW)], r_x.at[:, k, e],
                      x_ssem, x_rsem, dev(*row[k]))

    def y_copy(g, k, e):
        bb, _, cc = col[k]
        start, width = GROUPS[g]
        return remote(y_send.at[e, bb, :, cc, :, pl.ds(start, width)],
                      r_y.at[:, k, e, :, pl.ds(start - XW, width)],
                      y_ssem, y_rsem.at[g], dev(*col[k]))

    def z_copy(g):
        start, width = GROUPS[g]
        cols = pl.ds(start - XW, width)
        return remote(z_send.at[:, cols], z_recv.at[:, cols], z_ssem, z_rsem.at[g], x_partner)

    w_copy = remote(w_send, w_recv, w_ssem, w_rsem, y_partner)
    tok_copies = [remote(tok, tok_r.at[0], tok_ssem, tok_rsem.at[0], x_partner),
                  remote(tok, tok_r.at[1], tok_ssem, tok_rsem.at[1], y_partner)]

    def half_copies(n):
        cols = pl.ds(n * TILE, TILE)
        return (pltpu.make_async_copy(wg_hbm.at[0, :, cols], wg_v.at[0, :, cols], half_sems.at[0, n]),
                pltpu.make_async_copy(wu_hbm.at[0, :, cols], wu_v.at[0, :, cols], half_sems.at[1, n]))

    halves = wg_v.shape[2] // TILE
    map_copies = [pltpu.make_async_copy(src, dst, map_sems.at[i]) for i, (src, dst) in enumerate(
        ((slot_hbm, slot_ref), (ids_hbm, ids_ref), (gate_hbm, gate_ref)))]
    rows_in(0).start()
    for n in range(halves):
        for cp in half_copies(n):
            cp.start()
    down_in(0).start()
    for cp in map_copies:
        cp.start()

    barrier = pltpu.get_barrier_semaphore()
    for peer in (row[1], row[2], row[3], col[2], col[3]):
        pl.semaphore_signal(barrier, inc=1, device_id=dev(*peer), device_id_type=pl.DeviceIdType.MESH)

    def load_maps():
        for cp in map_copies:
            cp.wait()
        slot = slot_ref[...]
        flat = jnp.where(slot >= 0, ids_ref[...] * cap + slot, -1).astype(jnp.float32)
        tok[...] = jnp.full(tok.shape, -1.0, jnp.float32)
        tok[0:8, 0:toks] = flat
        tok[8:16, 0:toks] = gate_ref[...]

    def start_in(e):
        for cp in in_copies(e):
            cp.start()

    def up(e, n):
        xs = x_v[e].reshape(8 * cap, x_v.shape[3])
        g = jnp.dot(xs, wg_v[e, :, n:n + TILE], preferred_element_type=jnp.float32)
        u = jnp.dot(xs, wu_v[e, :, n:n + TILE], preferred_element_type=jnp.float32)
        h_v[:, n:n + TILE] = (jax.nn.silu(g) * u).astype(jnp.bfloat16)

    def down_and_send(e):
        h = h_v[...]
        sent = 0
        for n in range(0, y_send.shape[5], TILE):
            y = jnp.dot(h, wd_v[e, :, n:n + TILE], preferred_element_type=jnp.float32)
            y_send[e, :, :, :, :, n:n + TILE] = y.astype(jnp.bfloat16).reshape(2, 2, 2, cap, TILE)
            if sent == 0 and n + TILE >= XW:
                for k in (2, 3, 1):
                    x_copy(k, e).start()
                sent = 1
            if sent == 1 and n + TILE >= GROUPS[0][0] + GROUPS[0][1]:
                for k in (2, 3, 1):
                    y_copy(0, k, e).start()
                sent = 2
        r_x[:, 0, e] = y_send[e, :, x, c, :, 0:XW]
        r_y[:, 0, e] = y_send[e, b, :, c, :, XW:]

    rows_in(0).wait()
    for n in range(halves):
        for cp in half_copies(n):
            cp.wait()
        if n == 0:
            start_in(1)
        up(0, n * TILE)
        if n == 0:
            load_maps()
    with jax.named_scope('barrier'):
        pl.semaphore_wait(barrier, 5)
    for cp in tok_copies:
        cp.start()
    down_in(0).wait()
    start_in(2)
    down_and_send(0)

    def ffn(e, carry):
        with jax.named_scope('in_wait'):
            for cp in in_copies(e):
                cp.wait()

        @pl.when(e + 2 < experts)
        def _():
            start_in(e + 2)

        for n in range(0, h_v.shape[1], TILE):
            up(e, n)
        down_and_send(e)
        return carry

    lax.fori_loop(1, experts, ffn, 0)

    for g in range(1, len(GROUPS)):
        for e in range(experts):
            for k in (2, 3, 1):
                y_copy(g, k, e).start()

    def build(i, tok_val, devices):
        rows = lax.broadcasted_iota(jnp.int32, (blk, tok_val.shape[1]), 0)
        for k in range(4):
            bb, xx, cc = devices[k]
            want = (rows + blk * (4 * bb + 2 * xx + cc)).astype(jnp.float32)
            s = jnp.zeros(want.shape, jnp.float32)
            for j in range(8):
                s = s + jnp.where(tok_val[j:j + 1, :] == want, tok_val[8 + j:9 + j, :], 0.0)
            st_f32[k * blk:(k + 1) * blk, :] = s
            hit = jnp.max(s, axis=1, keepdims=True)
            used[i, k * blk:(k + 1) * blk, :] = jnp.broadcast_to(
                jnp.where(hit > 0.0, 1.0, 0.0), (blk, 128)).astype(jnp.bfloat16)
        for m in range(0, 4 * blk, 128):
            t = jnp.transpose(st_f32[m:m + 128, :])[0:toks, :]
            s1 = jnp.minimum(t, BF16_MAX).astype(jnp.bfloat16)
            t = t - s1.astype(jnp.float32)
            s2 = t.astype(jnp.bfloat16)
            s3 = (t - s2.astype(jnp.float32)).astype(jnp.bfloat16)
            s_mat[i, 0:toks, m:m + 128] = s1
            s_mat[i, toks:2 * toks, m:m + 128] = s2
            s_mat[i, 2 * toks:3 * toks, m:m + 128] = s3

    def combine(i, rows, start, write):
        width = rows.shape[4]
        for n in range(0, width, 128):
            r = rows[:, :, :, :, n:n + 128].reshape(4 * blk, 128)
            r = jnp.where(used[i] > 0, r, jnp.zeros_like(r))
            o = jnp.dot(s_mat[i], r, preferred_element_type=jnp.float32)
            write(start + n, o[0:toks] + o[toks:2 * toks] + o[2 * toks:3 * toks])

    with jax.named_scope('build'):
        for cp in tok_copies:
            cp.wait_recv()
        build(0, tok_r[0], col)
        build(1, tok[...], col)
        build(2, tok_r[1], row)
        build(3, tok[...], row)

    def put_z(n, v):
        z_send[:, n:n + 128] = v

    def put_w(n, v):
        w_send[:, n:n + 128] = v.astype(jnp.bfloat16)

    def put_acc(n, v):
        acc[:, n:n + 128] = v

    def y_group(g):
        start, width = GROUPS[g]
        cols = pl.ds(start - XW, width)
        with jax.named_scope(f'y_wait{g}'):
            drain(r_y.at[:, others, :, :, cols], y_rsem.at[g])
        with jax.named_scope(f'y_comb{g}'):
            combine(0, r_y.at[pl.ds(1 - x, 1), :, :, :, cols], start - XW, put_z)
            z_copy(g).start()
        with jax.named_scope(f'y_own{g}'):
            combine(1, r_y.at[pl.ds(x, 1), :, :, :, cols], start, put_acc)

    y_group(0)
    y_group(1)
    with jax.named_scope('x_wait'):
        drain(r_x.at[:, others], x_rsem)
    combine(2, r_x.at[pl.ds(1 - b, 1)], 0, put_w)
    w_copy.start()
    combine(3, r_x.at[pl.ds(b, 1)], 0, put_acc)
    y_group(2)

    y_group(3)

    def finish(g):
        start, width = GROUPS[g]
        with jax.named_scope(f'z_wait{g}'):
            z_copy(g).wait_recv()
        out_ref[:, start:start + width] = (
            acc[:, start:start + width] + z_recv[:, start - XW:start - XW + width]).astype(jnp.bfloat16)

    finish(0)
    finish(1)
    finish(2)
    with jax.named_scope('w_wait'):
        w_copy.wait_recv()
    out_ref[:, 0:XW] = (acc[:, 0:XW] + w_recv[...].astype(jnp.float32)).astype(jnp.bfloat16)
    finish(3)

    drain(tok_r, tok_ssem)
    drain(r_x.at[:, others], x_ssem)
    drain(r_y.at[:, others], y_ssem)
    drain(z_send, z_ssem)
    w_copy.wait_send()


def solution(mesh):
    def local_step(x_disp, w_gate, w_up, w_down, slot_idx, expert_ids, gate_wts):
        sources, experts, cap, width = x_disp.shape
        ff = w_gate.shape[2]
        toks = slot_idx.shape[0]
        yw = width - XW
        ng = len(GROUPS)
        dma = pltpu.SemaphoreType.DMA
        bf16, f32 = jnp.bfloat16, jnp.float32
        vmem = pl.BlockSpec(memory_space=pltpu.VMEM)
        hbm = pl.BlockSpec(memory_space=pl.ANY)
        rows = 4 * experts * cap
        return pl.pallas_call(
            kernel,
            out_shape=pltpu.VMEM((toks, width), bf16),
            in_specs=[hbm] * 7,
            out_specs=vmem,
            scratch_shapes=[
                pltpu.VMEM((8, toks), jnp.int32),
                pltpu.VMEM((8, toks), jnp.int32),
                pltpu.VMEM((8, toks), f32),
                pltpu.VMEM((experts, sources, cap, width), bf16),
                pltpu.VMEM((experts, width, ff), bf16),
                pltpu.VMEM((experts, width, ff), bf16),
                pltpu.VMEM((experts, ff, width), bf16),
                pltpu.VMEM((sources * cap, ff), bf16),
                pltpu.VMEM((experts, 2, 2, 2, cap, width), bf16),
                pltpu.VMEM((2, 4, experts, cap, XW), bf16),
                pltpu.VMEM((2, 4, experts, cap, yw), bf16),
                pltpu.VMEM((16, 256), f32),
                pltpu.VMEM((2, 16, 256), f32),
                pltpu.VMEM((rows, 256), f32),
                pltpu.VMEM((4, 3 * toks, rows), bf16),
                pltpu.VMEM((4, rows, 128), bf16),
                pltpu.VMEM((toks, yw), f32),
                pltpu.VMEM((toks, yw), f32),
                pltpu.VMEM((toks, XW), bf16),
                pltpu.VMEM((toks, XW), bf16),
                pltpu.VMEM((toks, width), f32),
                dma((4, 2)), dma((2, ff // TILE)), dma((3,)), dma, dma((2,)),
                dma, dma, dma, dma((ng,)), dma, dma((ng,)), dma, dma,
            ],
            compiler_params=pltpu.CompilerParams(
                collective_id=0, has_side_effects=True, vmem_limit_bytes=60 * 2**20),
            name="moe",
        )(x_disp, w_gate, w_up, w_down, slot_idx.T, expert_ids.T, gate_wts.T)

    expert_spec = P(("outer", "expert"))
    token_spec = P(("data", "outer", "expert"))
    return jax.shard_map(local_step, mesh=mesh, in_specs=(P("data", ("outer", "expert")), expert_spec, expert_spec, expert_spec, token_spec, token_spec, token_spec), out_specs=token_spec, check_vma=False)
```

```python
import functools

import jax
import jax.numpy as jnp
from jax import lax
from jax.experimental import pallas as pl
from jax.experimental.pallas import tpu as pltpu
from jax.sharding import PartitionSpec as P

XW = 640
TILE = 256
STEP = 512
K_STEP = 256
Z_LAST = 128
BF16_MAX = 3.3895313892515355e38


def kernel(x_hbm, wg_hbm, wu_hbm, wd_hbm, slot_hbm, ids_hbm, gate_hbm, out_ref,
           slot_ref, ids_ref, gate_ref, x_v, wg_v, wu_v, wd_v, g_v, u_v, h_v, y_send, r_x, r_y, tok, tok_r, st_f32,
           s_mat, used, z_send, z_recv, w_send, w_recv, acc,
           in_sems, first_sems, map_sems, tok_ssem, tok_rsem, x_ssem, x_rsem, y_ssem, y_rsem,
           z_ssem, z_rsem, w_ssem, w_rsem):
    b = lax.axis_index("outer")
    q = lax.axis_index("expert")
    x = q // 2
    c = q % 2
    experts = x_v.shape[0]
    cap = x_v.shape[2]
    blk = experts * cap
    toks, width = out_ref.shape

    def dev(bb, xx, cc):
        return {"outer": bb, "expert": 2 * xx + cc}

    row = [(b, x, c), (b, x, 1 - c), (b, 1 - x, c), (b, 1 - x, 1 - c)]
    col = [(b, x, c), (b, x, 1 - c), (1 - b, x, c), (1 - b, x, 1 - c)]
    x_partner = dev(b, 1 - x, c)
    y_partner = dev(1 - b, x, c)

    def rows_in(e):
        return pltpu.make_async_copy(x_hbm.at[:, e], x_v.at[e], in_sems.at[0, e % 2])

    def down_in(e):
        return pltpu.make_async_copy(wd_hbm.at[e], wd_v.at[e], in_sems.at[3, e % 2])

    def up_copies(e):
        return (rows_in(e),
                pltpu.make_async_copy(wg_hbm.at[e], wg_v.at[e], in_sems.at[1, e % 2]),
                pltpu.make_async_copy(wu_hbm.at[e], wu_v.at[e], in_sems.at[2, e % 2]))

    def start_in(e):
        for cp in up_copies(e):
            cp.start()
        down_in(e).start()

    def remote(src, dst, ssem, rsem, device):
        return pltpu.make_async_remote_copy(
            src_ref=src, dst_ref=dst, send_sem=ssem, recv_sem=rsem,
            device_id=device, device_id_type=pl.DeviceIdType.MESH)

    def drain(ref, sem):
        pltpu.make_async_copy(ref, ref, sem).wait()

    others = pl.ds(1, 3)

    def x_copy(k, e, start=0, stop=XW):
        _, xx, cc = row[k]
        cols = pl.ds(start, stop - start)
        return remote(y_send.at[e, :, xx, cc, :, cols], r_x.at[:, k, e, :, cols],
                      x_ssem, x_rsem, dev(*row[k]))

    def y_copy(own, k, e, start, stop):
        bb, _, cc = col[k]
        xx = x if own else 1 - x
        return remote(y_send.at[e, bb, xx, cc, :, pl.ds(start, stop - start)],
                      r_y.at[xx, k, e, :, pl.ds(start - XW, stop - start)],
                      y_ssem, y_rsem.at[own], dev(*col[k]))

    yw = z_send.shape[1]
    z_parts = [(0, yw - Z_LAST), (yw - Z_LAST, Z_LAST)]

    def z_copy(g):
        cols = pl.ds(*z_parts[g])
        return remote(z_send.at[:, cols], z_recv.at[:, cols], z_ssem, z_rsem.at[g], x_partner)

    w_copy = remote(w_send, w_recv, w_ssem, w_rsem, y_partner)
    tok_copies = [remote(tok, tok_r.at[0], tok_ssem, tok_rsem.at[0], x_partner),
                  remote(tok, tok_r.at[1], tok_ssem, tok_rsem.at[1], y_partner)]

    def first_up(m):
        ks = pl.ds(m * K_STEP, K_STEP)
        return (pltpu.make_async_copy(x_hbm.at[:, 0, :, ks], x_v.at[0, :, :, ks], first_sems.at[0, m]),
                pltpu.make_async_copy(wg_hbm.at[0, ks], wg_v.at[0, ks], first_sems.at[1, m]),
                pltpu.make_async_copy(wu_hbm.at[0, ks], wu_v.at[0, ks], first_sems.at[2, m]))

    def first_down(m):
        cols = pl.ds(m * STEP, STEP)
        return pltpu.make_async_copy(wd_hbm.at[0, :, cols], wd_v.at[0, :, cols], first_sems.at[3, m])

    steps = wg_v.shape[1] // K_STEP
    map_copies = [pltpu.make_async_copy(src, dst, map_sems.at[i]) for i, (src, dst) in enumerate(
        ((slot_hbm, slot_ref), (ids_hbm, ids_ref), (gate_hbm, gate_ref)))]
    for m in range(steps):
        for cp in first_up(m):
            cp.start()
    for m in range(width // STEP):
        first_down(m).start()
    for cp in map_copies:
        cp.start()
    start_in(1)

    barrier = pltpu.get_barrier_semaphore()
    for peer in (row[1], row[2], row[3], col[2], col[3]):
        pl.semaphore_signal(barrier, inc=1, device_id=dev(*peer), device_id_type=pl.DeviceIdType.MESH)

    def load_maps():
        for cp in map_copies:
            cp.wait()
        slot = slot_ref[...]
        flat = jnp.where(slot >= 0, ids_ref[...] * cap + slot, -1).astype(jnp.float32)
        tok[...] = jnp.full(tok.shape, -1.0, jnp.float32)
        tok[0:8, 0:toks] = flat
        tok[8:16, 0:toks] = gate_ref[...]


    def up(e, n):
        xs = x_v[e].reshape(8 * cap, x_v.shape[3])
        g = jnp.dot(xs, wg_v[e, :, n:n + TILE], preferred_element_type=jnp.float32)
        u = jnp.dot(xs, wu_v[e, :, n:n + TILE], preferred_element_type=jnp.float32)
        h_v[:, n:n + TILE] = (jax.nn.silu(g) * u).astype(jnp.bfloat16)

    def down(e, n):
        y = jnp.dot(h_v[...], wd_v[e, :, n:n + STEP], preferred_element_type=jnp.float32)
        y_send[e, :, :, :, :, n:n + STEP] = y.astype(jnp.bfloat16).reshape(2, 2, 2, cap, STEP)

    def keep_own(e):
        r_x[:, 0, e] = y_send[e, :, x, c, :, 0:XW]
        r_y[:, 0, e] = y_send[e, b, :, c, :, XW:]

    def send_x(e, start, stop):
        for k in (2, 3, 1):
            x_copy(k, e, start, stop).start()

    def send_y(own, e, start, stop):
        for k in (2, 3, 1):
            y_copy(own, k, e, start, stop).start()

    for m in range(steps):
        with jax.named_scope(f'f_wait{m}'):
            for cp in first_up(m):
                cp.wait()
        with jax.named_scope(f'f_up{m}'):
            ks = slice(m * K_STEP, (m + 1) * K_STEP)
            rows = x_v[0, :, :, ks].reshape(8 * cap, K_STEP)
            for n in range(0, h_v.shape[1], TILE):
                cols = slice(n, n + TILE)
                g = jnp.dot(rows, wg_v[0, ks, cols], preferred_element_type=jnp.float32)
                u = jnp.dot(rows, wu_v[0, ks, cols], preferred_element_type=jnp.float32)
                if m > 0:
                    g = g_v[:, cols] + g
                    u = u_v[:, cols] + u
                if m < steps - 1:
                    g_v[:, cols] = g
                    u_v[:, cols] = u
                else:
                    h_v[:, cols] = (jax.nn.silu(g) * u).astype(jnp.bfloat16)
    with jax.named_scope('down0'):
        first_down(0).wait()
        down(0, 0)
    with jax.named_scope('barrier'):
        pl.semaphore_wait(barrier, 5)
    send_x(0, 0, STEP)
    with jax.named_scope('down1'):
        first_down(1).wait()
        down(0, STEP)
        send_x(0, STEP, XW)
        send_y(0, 0, XW, 2 * STEP)
    with jax.named_scope('down2'):
        first_down(2).wait()
        start_in(2)
        down(0, 2 * STEP)
        send_y(0, 0, 2 * STEP, width)
    load_maps()
    keep_own(0)
    for cp in tok_copies:
        cp.start()

    def ffn(e, carry):
        with jax.named_scope('in_wait'):
            for cp in up_copies(e):
                cp.wait()
        for n in range(0, h_v.shape[1], TILE):
            up(e, n)
        with jax.named_scope('d_wait'):
            down_in(e).wait()

        @pl.when(e + 2 < experts)
        def _():
            start_in(e + 2)

        down(e, 0)
        send_x(e, 0, STEP)
        down(e, STEP)
        send_x(e, STEP, XW)
        send_y(0, e, XW, 2 * STEP)
        down(e, 2 * STEP)
        send_y(0, e, 2 * STEP, width)
        keep_own(e)
        return carry

    lax.fori_loop(1, experts, ffn, 0)

    for e in range(experts):
        send_y(1, e, XW, width)

    def build(i, tok_val, devices):
        rows = lax.broadcasted_iota(jnp.int32, (blk, tok_val.shape[1]), 0)
        for k in range(4):
            bb, xx, cc = devices[k]
            want = (rows + blk * (4 * bb + 2 * xx + cc)).astype(jnp.float32)
            s = jnp.zeros(want.shape, jnp.float32)
            for j in range(8):
                s = s + jnp.where(tok_val[j:j + 1, :] == want, tok_val[8 + j:9 + j, :], 0.0)
            st_f32[k * blk:(k + 1) * blk, :] = s
            hit = jnp.max(s, axis=1, keepdims=True)
            used[i, k * blk:(k + 1) * blk, :] = jnp.broadcast_to(
                jnp.where(hit > 0.0, 1.0, 0.0), (blk, 128)).astype(jnp.bfloat16)
        for m in range(0, 4 * blk, 128):
            t = jnp.transpose(st_f32[m:m + 128, :])[0:toks, :]
            s1 = jnp.minimum(t, BF16_MAX).astype(jnp.bfloat16)
            t = t - s1.astype(jnp.float32)
            s2 = t.astype(jnp.bfloat16)
            s3 = (t - s2.astype(jnp.float32)).astype(jnp.bfloat16)
            s_mat[i, 0:toks, m:m + 128] = s1
            s_mat[i, toks:2 * toks, m:m + 128] = s2
            s_mat[i, 2 * toks:3 * toks, m:m + 128] = s3

    def combine(i, rows, start, stop, write):
        for n in range(start, stop, 128):
            r = rows[:, :, :, n:n + 128].reshape(4 * blk, 128)
            r = jnp.where(used[i] > 0, r, jnp.zeros_like(r))
            o = jnp.dot(s_mat[i], r, preferred_element_type=jnp.float32)
            write(n, o[0:toks] + o[toks:2 * toks] + o[2 * toks:3 * toks])

    with jax.named_scope('build'):
        for cp in tok_copies:
            cp.wait_recv()
        build(0, tok_r[0], col)
        build(1, tok[...], col)
        build(2, tok_r[1], row)
        build(3, tok[...], row)

    def put_z(n, v):
        z_send[:, n:n + 128] = v

    def put_w(n, v):
        w_send[:, n:n + 128] = v.astype(jnp.bfloat16)

    def put_x(n, v):
        acc[:, n:n + 128] = v

    def put_y(n, v):
        acc[:, XW + n:XW + n + 128] = v

    with jax.named_scope('y_wait'):
        drain(r_y.at[1 - x, others], y_rsem.at[0])
    with jax.named_scope('y_comb'):
        for g, (start, size) in enumerate(z_parts):
            combine(0, r_y.at[1 - x], start, start + size, put_z)
            z_copy(g).start()
    with jax.named_scope('x_wait'):
        drain(r_x.at[:, others], x_rsem)
    with jax.named_scope('x_comb'):
        combine(2, r_x.at[1 - b], 0, XW, put_w)
        w_copy.start()
    with jax.named_scope('x_own'):
        combine(3, r_x.at[b], 0, XW, put_x)
    with jax.named_scope('o_wait'):
        drain(r_y.at[x, others], y_rsem.at[1])
    with jax.named_scope('y_own'):
        combine(1, r_y.at[x], 0, yw, put_y)

    def finish(g):
        start, size = z_parts[g]
        with jax.named_scope(f'z_wait{g}'):
            z_copy(g).wait_recv()
        out_ref[:, XW + start:XW + start + size] = (
            acc[:, XW + start:XW + start + size] + z_recv[:, start:start + size]).astype(jnp.bfloat16)

    for g in range(len(z_parts) - 1):
        finish(g)
    with jax.named_scope('w_wait'):
        w_copy.wait_recv()
    out_ref[:, 0:XW] = (acc[:, 0:XW] + w_recv[...].astype(jnp.float32)).astype(jnp.bfloat16)
    finish(len(z_parts) - 1)

    drain(tok_r, tok_ssem)
    drain(r_x.at[:, others], x_ssem)
    drain(r_y.at[:, others], y_ssem)
    drain(z_send, z_ssem)
    w_copy.wait_send()


def solution(mesh):
    def local_step(x_disp, w_gate, w_up, w_down, slot_idx, expert_ids, gate_wts):
        sources, experts, cap, width = x_disp.shape
        ff = w_gate.shape[2]
        toks = slot_idx.shape[0]
        yw = width - XW
        dma = pltpu.SemaphoreType.DMA
        bf16, f32 = jnp.bfloat16, jnp.float32
        vmem = pl.BlockSpec(memory_space=pltpu.VMEM)
        hbm = pl.BlockSpec(memory_space=pl.ANY)
        rows = 4 * experts * cap
        return pl.pallas_call(
            kernel,
            out_shape=pltpu.VMEM((toks, width), bf16),
            in_specs=[hbm] * 7,
            out_specs=vmem,
            scratch_shapes=[
                pltpu.VMEM((8, toks), jnp.int32),
                pltpu.VMEM((8, toks), jnp.int32),
                pltpu.VMEM((8, toks), f32),
                pltpu.VMEM((experts, sources, cap, width), bf16),
                pltpu.VMEM((experts, width, ff), bf16),
                pltpu.VMEM((experts, width, ff), bf16),
                pltpu.VMEM((experts, ff, width), bf16),
                pltpu.VMEM((sources * cap, ff), f32),
                pltpu.VMEM((sources * cap, ff), f32),
                pltpu.VMEM((sources * cap, ff), bf16),
                pltpu.VMEM((experts, 2, 2, 2, cap, width), bf16),
                pltpu.VMEM((2, 4, experts, cap, XW), bf16),
                pltpu.VMEM((2, 4, experts, cap, yw), bf16),
                pltpu.VMEM((16, 256), f32),
                pltpu.VMEM((2, 16, 256), f32),
                pltpu.VMEM((rows, 256), f32),
                pltpu.VMEM((4, 3 * toks, rows), bf16),
                pltpu.VMEM((4, rows, 128), bf16),
                pltpu.VMEM((toks, yw), f32),
                pltpu.VMEM((toks, yw), f32),
                pltpu.VMEM((toks, XW), bf16),
                pltpu.VMEM((toks, XW), bf16),
                pltpu.VMEM((toks, width), f32),
                dma((4, 2)), dma((4, width // K_STEP)), dma((3,)), dma, dma((2,)),
                dma, dma, dma, dma((2,)), dma, dma((2,)), dma, dma,
            ],
            compiler_params=pltpu.CompilerParams(
                collective_id=0, has_side_effects=True, vmem_limit_bytes=60 * 2**20),
            name="moe",
        )(x_disp, w_gate, w_up, w_down, slot_idx.T, expert_ids.T, gate_wts.T)

    expert_spec = P(("outer", "expert"))
    token_spec = P(("data", "outer", "expert"))
    return jax.shard_map(local_step, mesh=mesh, in_specs=(P("data", ("outer", "expert")), expert_spec, expert_spec, expert_spec, token_spec, token_spec, token_spec), out_specs=token_spec, check_vma=False)
```

```python
import functools

import jax
import jax.numpy as jnp
from jax import lax
from jax.experimental import pallas as pl
from jax.experimental.pallas import tpu as pltpu
from jax.sharding import PartitionSpec as P

XW = 640
TILE = 256
STEP = 512
K_STEP = 256
Z_LAST = 128
BF16_MAX = 3.3895313892515355e38


def kernel(x_hbm, wg_hbm, wu_hbm, wd_hbm, slot_hbm, ids_hbm, gate_hbm, out_ref,
           slot_ref, ids_ref, gate_ref, x_v, wg_v, wu_v, wd_v, g_v, u_v, h_v, y_send, r_x, r_y, tok, tok_r, st_f32,
           s_mat, used, z_send, z_recv, w_send, w_recv, acc,
           in_sems, first_sems, map_sems, tok_ssem, tok_rsem, x_ssem, x_rsem, y_ssem, y_rsem,
           z_ssem, z_rsem, w_ssem, w_rsem):
    b = lax.axis_index("outer")
    q = lax.axis_index("expert")
    x = q // 2
    c = q % 2
    experts = x_v.shape[0]
    cap = x_v.shape[2]
    blk = experts * cap
    toks, width = out_ref.shape

    def dev(bb, xx, cc):
        return {"outer": bb, "expert": 2 * xx + cc}

    row = [(b, x, c), (b, x, 1 - c), (b, 1 - x, c), (b, 1 - x, 1 - c)]
    col = [(b, x, c), (b, x, 1 - c), (1 - b, x, c), (1 - b, x, 1 - c)]
    x_partner = dev(b, 1 - x, c)
    y_partner = dev(1 - b, x, c)

    def rows_in(e):
        return pltpu.make_async_copy(x_hbm.at[:, e], x_v.at[e], in_sems.at[0, e % 2])

    def down_in(e):
        return pltpu.make_async_copy(wd_hbm.at[e], wd_v.at[e], in_sems.at[3, e % 2])

    def up_copies(e):
        return (rows_in(e),
                pltpu.make_async_copy(wg_hbm.at[e], wg_v.at[e], in_sems.at[1, e % 2]),
                pltpu.make_async_copy(wu_hbm.at[e], wu_v.at[e], in_sems.at[2, e % 2]))

    def start_in(e):
        for cp in up_copies(e):
            cp.start()
        down_in(e).start()

    def remote(src, dst, ssem, rsem, device):
        return pltpu.make_async_remote_copy(
            src_ref=src, dst_ref=dst, send_sem=ssem, recv_sem=rsem,
            device_id=device, device_id_type=pl.DeviceIdType.MESH)

    def drain(ref, sem):
        pltpu.make_async_copy(ref, ref, sem).wait()

    others = pl.ds(1, 3)

    def x_copy(k, e, start=0, stop=XW):
        _, xx, cc = row[k]
        cols = pl.ds(start, stop - start)
        return remote(y_send.at[e, :, xx, cc, :, cols], r_x.at[:, k, e, :, cols],
                      x_ssem, x_rsem, dev(*row[k]))

    def y_copy(own, k, e, start, stop):
        bb, _, cc = col[k]
        xx = x if own else 1 - x
        return remote(y_send.at[e, bb, xx, cc, :, pl.ds(start, stop - start)],
                      r_y.at[xx, k, e, :, pl.ds(start - XW, stop - start)],
                      y_ssem, y_rsem.at[own], dev(*col[k]))

    yw = z_send.shape[1]
    z_parts = [(0, yw - Z_LAST), (yw - Z_LAST, Z_LAST)]

    def z_copy(g):
        cols = pl.ds(*z_parts[g])
        return remote(z_send.at[:, cols], z_recv.at[:, cols], z_ssem, z_rsem.at[g], x_partner)

    w_copy = remote(w_send, w_recv, w_ssem, w_rsem, y_partner)
    tok_copies = [remote(tok, tok_r.at[0], tok_ssem, tok_rsem.at[0], x_partner),
                  remote(tok, tok_r.at[1], tok_ssem, tok_rsem.at[1], y_partner)]

    def first_up(m):
        ks = pl.ds(m * K_STEP, K_STEP)
        return (pltpu.make_async_copy(x_hbm.at[:, 0, :, ks], x_v.at[0, :, :, ks], first_sems.at[0, m]),
                pltpu.make_async_copy(wg_hbm.at[0, ks], wg_v.at[0, ks], first_sems.at[1, m]),
                pltpu.make_async_copy(wu_hbm.at[0, ks], wu_v.at[0, ks], first_sems.at[2, m]))

    edges = (0, 256, 768, 1280, 1536)
    pieces = tuple(zip(edges[:-1], edges[1:]))

    def first_down(m):
        cols = pl.ds(pieces[m][0], pieces[m][1] - pieces[m][0])
        return pltpu.make_async_copy(wd_hbm.at[0, :, cols], wd_v.at[0, :, cols], first_sems.at[3, m])

    steps = wg_v.shape[1] // K_STEP
    map_copies = [pltpu.make_async_copy(src, dst, map_sems.at[i]) for i, (src, dst) in enumerate(
        ((slot_hbm, slot_ref), (ids_hbm, ids_ref), (gate_hbm, gate_ref)))]
    for m in range(steps):
        for cp in first_up(m):
            cp.start()
    for m in range(len(pieces)):
        first_down(m).start()
    for cp in map_copies:
        cp.start()
    start_in(1)

    barrier = pltpu.get_barrier_semaphore()
    for peer in (row[1], row[2], row[3], col[2], col[3]):
        pl.semaphore_signal(barrier, inc=1, device_id=dev(*peer), device_id_type=pl.DeviceIdType.MESH)

    def load_maps():
        for cp in map_copies:
            cp.wait()
        slot = slot_ref[...]
        flat = jnp.where(slot >= 0, ids_ref[...] * cap + slot, -1).astype(jnp.float32)
        tok[...] = jnp.full(tok.shape, -1.0, jnp.float32)
        tok[0:8, 0:toks] = flat
        tok[8:16, 0:toks] = gate_ref[...]


    def up(e, n):
        xs = x_v[e].reshape(8 * cap, x_v.shape[3])
        g = jnp.dot(xs, wg_v[e, :, n:n + TILE], preferred_element_type=jnp.float32)
        u = jnp.dot(xs, wu_v[e, :, n:n + TILE], preferred_element_type=jnp.float32)
        h_v[:, n:n + TILE] = (jax.nn.silu(g) * u).astype(jnp.bfloat16)

    def down(e, start, stop):
        y = jnp.dot(h_v[...], wd_v[e, :, start:stop], preferred_element_type=jnp.float32)
        y_send[e, :, :, :, :, start:stop] = y.astype(jnp.bfloat16).reshape(2, 2, 2, cap, stop - start)

    def keep_own(e):
        r_x[:, 0, e] = y_send[e, :, x, c, :, 0:XW]
        r_y[:, 0, e] = y_send[e, b, :, c, :, XW:]

    def send_x(e, start, stop):
        for k in (2, 3, 1):
            x_copy(k, e, start, stop).start()

    def send_y(own, e, start, stop):
        for k in (2, 3, 1):
            y_copy(own, k, e, start, stop).start()

    for m in range(steps):
        with jax.named_scope(f'f_wait{m}'):
            for cp in first_up(m):
                cp.wait()
        with jax.named_scope(f'f_up{m}'):
            ks = slice(m * K_STEP, (m + 1) * K_STEP)
            rows = x_v[0, :, :, ks].reshape(8 * cap, K_STEP)
            for n in range(0, h_v.shape[1], TILE):
                cols = slice(n, n + TILE)
                g = jnp.dot(rows, wg_v[0, ks, cols], preferred_element_type=jnp.float32)
                u = jnp.dot(rows, wu_v[0, ks, cols], preferred_element_type=jnp.float32)
                if m > 0:
                    g = g_v[:, cols] + g
                    u = u_v[:, cols] + u
                if m < steps - 1:
                    g_v[:, cols] = g
                    u_v[:, cols] = u
                else:
                    h_v[:, cols] = (jax.nn.silu(g) * u).astype(jnp.bfloat16)
    with jax.named_scope('down0'):
        first_down(0).wait()
        half = h_v.shape[0] // 2
        for i in range(2):
            y = jnp.dot(h_v[i * half:(i + 1) * half], wd_v[0, :, 0:TILE], preferred_element_type=jnp.float32)
            y_send[0, i, :, :, :, 0:TILE] = y.astype(jnp.bfloat16).reshape(2, 2, cap, TILE)
    with jax.named_scope('barrier'):
        pl.semaphore_wait(barrier, 5)
    send_x(0, 0, TILE)
    for m in range(1, len(pieces)):
        start, stop = pieces[m]
        first_down(m).wait()
        if m == 3:
            start_in(2)
        with jax.named_scope(f'down{m}'):
            down(0, start, stop)
            if start < XW:
                send_x(0, start, XW)
            send_y(0, 0, max(start, XW), stop)
    load_maps()
    keep_own(0)
    for cp in tok_copies:
        cp.start()

    def ffn(e, carry):
        with jax.named_scope('in_wait'):
            for cp in up_copies(e):
                cp.wait()
        for n in range(0, h_v.shape[1], TILE):
            up(e, n)
        with jax.named_scope('d_wait'):
            down_in(e).wait()

        @pl.when(e + 2 < experts)
        def _():
            start_in(e + 2)

        down(e, 0, STEP)
        send_x(e, 0, STEP)
        down(e, STEP, 2 * STEP)
        send_x(e, STEP, XW)
        send_y(0, e, XW, 2 * STEP)
        down(e, 2 * STEP, width)
        send_y(0, e, 2 * STEP, width)
        keep_own(e)
        return carry

    lax.fori_loop(1, experts, ffn, 0)

    for e in range(experts):
        send_y(1, e, XW, width)

    def build(i, tok_val, devices):
        rows = lax.broadcasted_iota(jnp.int32, (blk, tok_val.shape[1]), 0)
        for k in range(4):
            bb, xx, cc = devices[k]
            want = (rows + blk * (4 * bb + 2 * xx + cc)).astype(jnp.float32)
            s = jnp.zeros(want.shape, jnp.float32)
            for j in range(8):
                s = s + jnp.where(tok_val[j:j + 1, :] == want, tok_val[8 + j:9 + j, :], 0.0)
            st_f32[k * blk:(k + 1) * blk, :] = s
            hit = jnp.max(s, axis=1, keepdims=True)
            used[i, k * blk:(k + 1) * blk, :] = jnp.broadcast_to(
                jnp.where(hit > 0.0, 1.0, 0.0), (blk, 128)).astype(jnp.bfloat16)
        for m in range(0, 4 * blk, 128):
            t = jnp.transpose(st_f32[m:m + 128, :])[0:toks, :]
            s1 = jnp.minimum(t, BF16_MAX).astype(jnp.bfloat16)
            t = t - s1.astype(jnp.float32)
            s2 = t.astype(jnp.bfloat16)
            s3 = (t - s2.astype(jnp.float32)).astype(jnp.bfloat16)
            s_mat[i, 0:toks, m:m + 128] = s1
            s_mat[i, toks:2 * toks, m:m + 128] = s2
            s_mat[i, 2 * toks:3 * toks, m:m + 128] = s3

    def combine(i, rows, start, stop, write):
        for n in range(start, stop, 128):
            r = rows[:, :, :, n:n + 128].reshape(4 * blk, 128)
            r = jnp.where(used[i] > 0, r, jnp.zeros_like(r))
            o = jnp.dot(s_mat[i], r, preferred_element_type=jnp.float32)
            write(n, o[0:toks] + o[toks:2 * toks] + o[2 * toks:3 * toks])

    with jax.named_scope('build'):
        for cp in tok_copies:
            cp.wait_recv()
        build(0, tok_r[0], col)
        build(1, tok[...], col)
        build(2, tok_r[1], row)
        build(3, tok[...], row)

    def put_z(n, v):
        z_send[:, n:n + 128] = v

    def put_w(n, v):
        w_send[:, n:n + 128] = v.astype(jnp.bfloat16)

    def put_x(n, v):
        acc[:, n:n + 128] = v

    def put_y(n, v):
        acc[:, XW + n:XW + n + 128] = v

    with jax.named_scope('y_wait'):
        drain(r_y.at[1 - x, others], y_rsem.at[0])
    with jax.named_scope('y_comb'):
        for g, (start, size) in enumerate(z_parts):
            combine(0, r_y.at[1 - x], start, start + size, put_z)
            z_copy(g).start()
    with jax.named_scope('x_wait'):
        drain(r_x.at[:, others], x_rsem)
    with jax.named_scope('x_comb'):
        combine(2, r_x.at[1 - b], 0, XW, put_w)
        w_copy.start()
    with jax.named_scope('x_own'):
        combine(3, r_x.at[b], 0, XW, put_x)
    with jax.named_scope('o_wait'):
        drain(r_y.at[x, others], y_rsem.at[1])
    with jax.named_scope('y_own'):
        combine(1, r_y.at[x], 0, yw, put_y)

    def finish(g):
        start, size = z_parts[g]
        with jax.named_scope(f'z_wait{g}'):
            z_copy(g).wait_recv()
        out_ref[:, XW + start:XW + start + size] = (
            acc[:, XW + start:XW + start + size] + z_recv[:, start:start + size]).astype(jnp.bfloat16)

    for g in range(len(z_parts) - 1):
        finish(g)
    with jax.named_scope('w_wait'):
        w_copy.wait_recv()
    out_ref[:, 0:XW] = (acc[:, 0:XW] + w_recv[...].astype(jnp.float32)).astype(jnp.bfloat16)
    finish(len(z_parts) - 1)

    drain(tok_r, tok_ssem)
    drain(r_x.at[:, others], x_ssem)
    drain(r_y.at[:, others], y_ssem)
    drain(z_send, z_ssem)
    w_copy.wait_send()


def solution(mesh):
    def local_step(x_disp, w_gate, w_up, w_down, slot_idx, expert_ids, gate_wts):
        sources, experts, cap, width = x_disp.shape
        ff = w_gate.shape[2]
        toks = slot_idx.shape[0]
        yw = width - XW
        dma = pltpu.SemaphoreType.DMA
        bf16, f32 = jnp.bfloat16, jnp.float32
        vmem = pl.BlockSpec(memory_space=pltpu.VMEM)
        hbm = pl.BlockSpec(memory_space=pl.ANY)
        rows = 4 * experts * cap
        return pl.pallas_call(
            kernel,
            out_shape=pltpu.VMEM((toks, width), bf16),
            in_specs=[hbm] * 7,
            out_specs=vmem,
            scratch_shapes=[
                pltpu.VMEM((8, toks), jnp.int32),
                pltpu.VMEM((8, toks), jnp.int32),
                pltpu.VMEM((8, toks), f32),
                pltpu.VMEM((experts, sources, cap, width), bf16),
                pltpu.VMEM((experts, width, ff), bf16),
                pltpu.VMEM((experts, width, ff), bf16),
                pltpu.VMEM((experts, ff, width), bf16),
                pltpu.VMEM((sources * cap, ff), f32),
                pltpu.VMEM((sources * cap, ff), f32),
                pltpu.VMEM((sources * cap, ff), bf16),
                pltpu.VMEM((experts, 2, 2, 2, cap, width), bf16),
                pltpu.VMEM((2, 4, experts, cap, XW), bf16),
                pltpu.VMEM((2, 4, experts, cap, yw), bf16),
                pltpu.VMEM((16, 256), f32),
                pltpu.VMEM((2, 16, 256), f32),
                pltpu.VMEM((rows, 256), f32),
                pltpu.VMEM((4, 3 * toks, rows), bf16),
                pltpu.VMEM((4, rows, 128), bf16),
                pltpu.VMEM((toks, yw), f32),
                pltpu.VMEM((toks, yw), f32),
                pltpu.VMEM((toks, XW), bf16),
                pltpu.VMEM((toks, XW), bf16),
                pltpu.VMEM((toks, width), f32),
                dma((4, 2)), dma((4, width // K_STEP)), dma((3,)), dma, dma((2,)),
                dma, dma, dma, dma((2,)), dma, dma((2,)), dma, dma,
            ],
            compiler_params=pltpu.CompilerParams(
                collective_id=0, has_side_effects=True, vmem_limit_bytes=60 * 2**20),
            name="moe",
        )(x_disp, w_gate, w_up, w_down, slot_idx.T, expert_ids.T, gate_wts.T)

    expert_spec = P(("outer", "expert"))
    token_spec = P(("data", "outer", "expert"))
    return jax.shard_map(local_step, mesh=mesh, in_specs=(P("data", ("outer", "expert")), expert_spec, expert_spec, expert_spec, token_spec, token_spec, token_spec), out_specs=token_spec, check_vma=False)
```
